32 devices in a mesh: gx: 8 (over z, y), gy: 4 (over x, core).
Axes of the slice: x: 2, y: 2, z: 4, core: 2. Of those that a mesh axis runs over, the one named last changes fastest.
Arguments:
- basis: bfloat16 [40960, 120], P(('gx', 'gy')), may hold values from -0.03125 to 0.03125
- snapshots: bfloat16 [40960, 256], P(('gx', 'gy')), may hold values from -6 to 6
- derivatives: bfloat16 [40960, 256], P(('gx', 'gy')), may hold values from -24 to 24
- quad_pairs: int32 [2, 7260], replicated, may hold values from 0 to 119, as said below
- penalty: float32 [7381], replicated, may hold values from 0.5 to 8
Outputs:
- operator: float32 [120, 7381], replicated
The draws below stay inside these ranges and needn't reach their ends.
Inputs may be any that keep to these rules, and one draw needn't show every extreme that they name: `quad_pairs`: every pair (i, j) with 0 <= i <= j < 120 stands in exactly one column, in an order drawn from the seed.
All inputs are finite; a program needn't handle non-finite values.
Results may differ from the reference program's by a relative error of at most 0.0003.
Values sent between devices are 32-bit elements; how exact they have to be, the bound alone decides.
A program may use at most 64 MiB of HBM per device.

```python
import math
import jax
import jax.numpy as jnp
from jax import lax

R = 120
NQ = 7260
F = 7381
SNAPS = 256
ITERS = 2
NDOF = 40960


def draw_quad_pairs(key, part):
    first, second = jnp.triu_indices(R)
    order = jax.random.permutation(key, first.shape[0])
    return jnp.stack([first[order], second[order]]).astype(jnp.int32)


def block_scale(own_key, extent, cuts, smallest, largest):
    loudness = 1.0
    for axis_at, shards_of in cuts:
        draws = jax.random.uniform(jax.random.fold_in(jax.random.fold_in(own_key, 6), axis_at), (shards_of,), jnp.float32, smallest / len(cuts), largest / len(cuts))
        loudness = loudness * jnp.repeat(jnp.exp(draws), extent[axis_at] // shards_of).reshape((-1,) + (1,) * (len(extent) - 1 - axis_at))
    return loudness


def noise(key, shape, spread, most, pieces=(), kind=jnp.bfloat16):
    entries = spread * jax.random.normal(key, shape, jnp.float32)
    if pieces:
        entries = entries * block_scale(key, shape, pieces, -0.22, 0.18)
    return jnp.clip(entries, -most, most).astype(kind)


def setup_inputs(seed: int = 0) -> dict:
    splits = jax.random.split(jax.random.key(seed), 6)
    basis = noise(splits[0], (NDOF, R), NDOF ** -0.5, 0.03125, ((0, 32),))
    snapshots = noise(splits[1], (NDOF, SNAPS), 1.0, 6.0, ((0, 32),))
    derivatives = noise(splits[2], (NDOF, SNAPS), 4.0, 24.0, ((0, 32),))
    quad_pairs = draw_quad_pairs(jax.random.fold_in(splits[5], 71), 0)
    penalty = jnp.clip(jnp.exp(jax.random.uniform(splits[4], (F,), jnp.float32, math.log(0.5), math.log(8.0))), 0.5, 8.0)
    return {"basis": basis, "snapshots": snapshots, "derivatives": derivatives, "quad_pairs": quad_pairs, "penalty": penalty}


def feature_rows(index, coeffs, pairs):
    total = coeffs.shape[0]
    count = pairs.shape[1]
    linear = coeffs[jnp.clip(index - 1, 0, total - 1)]
    slot = jnp.clip(index - 1 - total, 0, count - 1)
    quad = coeffs[pairs[0, slot]] * coeffs[pairs[1, slot]]
    column = index[:, None]
    width = 1 + total + count
    return jnp.where(column == 0, jnp.float32(1.0), jnp.where(column <= total, linear, jnp.where(column < width, quad, jnp.float32(0.0)))).astype(jnp.float32)

def reference(basis, snapshots, derivatives, quad_pairs, penalty):
    dims = (((0,), (0,)), ((), ()))
    coeffs = lax.dot_general(basis, snapshots, dims, preferred_element_type=jnp.float32)
    rates = lax.dot_general(basis, derivatives, dims, preferred_element_type=jnp.float32)
    width = 1 + R + NQ
    data = feature_rows(jnp.arange(width, dtype=jnp.int32), coeffs, quad_pairs)
    snaps = snapshots.shape[1]
    inner = (((1,), (1,)), ((), ()))
    normal = lax.dot_general(data, data, inner, precision=lax.Precision.HIGHEST, preferred_element_type=jnp.float32) / snaps
    normal = normal + jnp.diag(penalty)
    target = lax.dot_general(data, rates, inner, precision=lax.Precision.HIGHEST, preferred_element_type=jnp.float32) / math.sqrt(snaps)
    solution = jnp.zeros_like(target)
    residual = target
    direction = target
    norm_now = lax.optimization_barrier(jnp.sum(residual * residual, axis=0))
    for step in range(ITERS):
        image = jnp.dot(normal, direction, precision=lax.Precision.HIGHEST, preferred_element_type=jnp.float32)
        alpha = norm_now / lax.optimization_barrier(jnp.sum(direction * image, axis=0))
        solution = solution + alpha * direction
        residual = residual - alpha * image
        norm_next = lax.optimization_barrier(jnp.sum(residual * residual, axis=0))
        direction = residual + norm_next / norm_now * direction
        norm_now = norm_next
    return solution.T
```

```python
import functools
import math

import jax
import jax.numpy as jnp
from jax import lax
from jax.experimental import pallas as pl
from jax.experimental.pallas import tpu as pltpu
from jax.sharding import PartitionSpec as P

MESH = pl.DeviceIdType.MESH
LANES = 128
TILE = 256
highest = lax.Precision.HIGHEST
VM = pl.BlockSpec(memory_space=pltpu.VMEM)


def dot(a, b, ca, cb, precision=None):
    return lax.dot_general(
        a, b, (((ca,), (cb,)), ((), ())), precision=precision, preferred_element_type=jnp.float32
    )


def reduce_kernel(gx, gy, basis_ref, snap_ref, deriv_ref, out_ref, part, recv, send1, recv1, send2, recv2):
    n = gx * gy
    me = lax.axis_index("gx") * gy + lax.axis_index("gy")
    order = basis_ref.shape[1]
    rows = part.shape[1]

    def where(k):
        other = lax.rem(me + k, n)
        return other, (other // gy, lax.rem(other, gy))

    barrier = pltpu.get_barrier_semaphore()

    def greet(k, c):
        _, at = where(k)
        pl.semaphore_signal(barrier, inc=1, device_id=at, device_id_type=MESH)
        return c

    lax.fori_loop(1, n, greet, 0)
    basis = basis_ref[...]
    padded = rows * n // 2
    for which, ref in enumerate((snap_ref, deriv_ref)):
        prod = dot(basis, ref[...], 0, 0)
        prod = jnp.concatenate([prod, jnp.zeros((padded - order, prod.shape[1]), jnp.float32)], axis=0)
        part[which * (n // 2):(which + 1) * (n // 2)] = prod.reshape(n // 2, rows, prod.shape[1])
    pl.semaphore_wait(barrier, n - 1)

    def scatter(k):
        other, at = where(k)
        return pltpu.make_async_remote_copy(
            src_ref=part.at[other], dst_ref=recv.at[me], send_sem=send1.at[k], recv_sem=recv1.at[k],
            device_id=at, device_id_type=MESH)

    def spread(k):
        _, at = where(k)
        return pltpu.make_async_remote_copy(
            src_ref=recv.at[me], dst_ref=out_ref.at[me], send_sem=send2.at[k], recv_sem=recv2.at[k],
            device_id=at, device_id_type=MESH)

    def start(make):
        def go(k, c):
            make(k).start()
            return c
        lax.fori_loop(1, n, go, 0)

    def finish(make):
        def go(k, c):
            make(k).wait()
            return c
        lax.fori_loop(1, n, go, 0)

    start(scatter)
    recv[me] = part[me]
    finish(scatter)

    def add(k, total):
        return total + recv[k]

    total = lax.fori_loop(0, n, add, jnp.zeros(recv.shape[1:], jnp.float32))
    recv[me] = total
    start(spread)
    out_ref[me] = total
    finish(spread)


def fit_kernel(order, ones_row, cr_ref, pairs_ref, pen_ref, out_ref, t_ref, w_ref, x_ref, sem):
    snaps = cr_ref.shape[1]
    half = cr_ref.shape[0] // 2
    padded = t_ref.shape[1]
    width = x_ref.shape[1]
    coeffs = cr_ref[0:half]
    g = cr_ref[half:half + order] * (1.0 / math.sqrt(snaps))
    sq = coeffs * coeffs
    ct = coeffs.T
    inner = dot(ct, coeffs, 1, 0, highest)
    inner2 = dot(sq.T, sq, 1, 0, highest)
    kernel = 1.0 + inner + 0.5 * (inner * inner + inner2)
    s1 = dot(g, kernel, 1, 0, highest)
    ks1 = dot(s1, kernel, 1, 0, highest) * (1.0 / snaps)
    lhs = jnp.concatenate([g, s1 * (1.0 / snaps)], axis=0)
    lhs_hi = lhs.astype(jnp.bfloat16)
    lhs_lo = (lhs - lhs_hi.astype(jnp.float32)).astype(jnp.bfloat16)
    lhs_both = jnp.concatenate([lhs_hi, lhs_lo], axis=0)
    table = jnp.where(lax.broadcasted_iota(jnp.int32, ct.shape, 1) == ones_row, 1.0, ct)

    def tile(at, carry):
        dpt, tt, tw = carry
        base = pl.multiple_of(at * TILE, TILE)
        cols = []
        for h in range(TILE // LANES):
            sl = pl.ds(pl.multiple_of(base + h * LANES, LANES), LANES)
            left = jnp.take_along_axis(
                table, jnp.broadcast_to(pairs_ref[0:1, sl], table.shape), axis=1, mode="promise_in_bounds")
            right = jnp.take_along_axis(
                table, jnp.broadcast_to(pairs_ref[1:2, sl], table.shape), axis=1, mode="promise_in_bounds")
            cols.append(left * right)
        d = jnp.concatenate(cols, axis=1)
        d_hi = d.astype(jnp.bfloat16)
        d_lo = (d - d_hi.astype(jnp.float32)).astype(jnp.bfloat16)
        both = dot(lhs_both, d_hi, 1, 0)
        tv = both[:2 * order] + both[2 * order:] + dot(lhs_hi, d_lo, 1, 0)
        t, v = tv[:order], tv[order:]
        sl = pl.ds(base, TILE)
        pt = pen_ref[0:1, sl] * t
        w = v + pt
        t_ref[:, sl] = t
        w_ref[:, sl] = w
        dpt = dpt + dot(d_hi, pt.astype(jnp.bfloat16), 1, 1)
        sq, cross = t * t, t * w
        for h in range(TILE // LANES):
            tt = tt + sq[:, h * LANES:(h + 1) * LANES]
            tw = tw + cross[:, h * LANES:(h + 1) * LANES]
        return dpt, tt, tw

    zero = jnp.zeros((order, LANES), jnp.float32)
    dpt, tt, tw = lax.fori_loop(
        0, padded // TILE, tile, (jnp.zeros((snaps, order), jnp.float32), zero, zero))
    tt = jnp.sum(tt, axis=1, keepdims=True)
    tw = jnp.sum(tw, axis=1, keepdims=True)
    alpha = tt / tw
    image = ks1 + jnp.pad(dpt, ((0, 0), (0, LANES - order))).T[:order]
    moved = s1 - alpha * image
    gram = jnp.sum(moved * moved, axis=1, keepdims=True) * (1.0 / snaps)
    group = 8 * max(d for d in range(1, 6) if order // 8 % d == 0)
    copies = []
    for at in range(0, order, group):
        rows = slice(at, at + group)
        a = alpha[rows]
        t, w = t_ref[rows, :], w_ref[rows, :]
        r = t - a * w
        rr = r * r
        weighted = jnp.sum(rr * pen_ref[0:1, :], axis=1, keepdims=True) + gram[rows]
        now = jnp.sum(rr, axis=1, keepdims=True)
        ratio = now / tt[rows]
        second = now / (weighted - ratio * now / a)
        x = (a + second * ratio) * t + second * r
        x_ref[rows, :] = x[:, :width]
        copy = pltpu.make_async_copy(x_ref.at[rows, :], out_ref.at[rows, :], sem.at[at // group])
        copy.start()
        copies.append(copy)
    for copy in copies:
        copy.wait()


def solution(mesh):
    gx, gy = mesh.shape["gx"], mesh.shape["gy"]
    n = gx * gy

    def on_device(basis, snapshots, derivatives, quad_pairs, penalty):
        order, snaps = basis.shape[1], snapshots.shape[1]
        count = quad_pairs.shape[1]
        width = 1 + order + count
        padded = -(-width // TILE) * TILE
        half = LANES
        rows = 2 * half // n
        f32 = jnp.float32
        total = pl.pallas_call(
            functools.partial(reduce_kernel, gx, gy),
            out_shape=jax.ShapeDtypeStruct((n, rows, snaps), f32),
            in_specs=[VM] * 3,
            out_specs=VM,
            scratch_shapes=[pltpu.VMEM((n, rows, snaps), f32)] * 2 + [pltpu.SemaphoreType.DMA((n,))] * 4,
            compiler_params=pltpu.CompilerParams(collective_id=0, has_side_effects=True),
            name="reduce",
        )(basis, snapshots, derivatives)
        linear = jnp.arange(order, dtype=jnp.int32)
        one = jnp.full((1,), order, jnp.int32)
        ones = jnp.full((order,), order, jnp.int32)
        tail = jnp.full((padded - width,), LANES - 1, jnp.int32)
        pairs = jnp.stack([
            jnp.concatenate([one, linear, quad_pairs[0], tail]),
            jnp.concatenate([one, ones, quad_pairs[1], tail]),
        ])
        weights = jnp.pad(penalty, (0, padded - width))[None, :]
        return pl.pallas_call(
            functools.partial(fit_kernel, order, order),
            out_shape=jax.ShapeDtypeStruct((order, width), f32),
            in_specs=[VM] * 3,
            out_specs=pl.BlockSpec(memory_space=pl.ANY),
            scratch_shapes=[
                pltpu.VMEM((order, padded), f32),
                pltpu.VMEM((order, padded), f32),
                pltpu.VMEM((order, width), f32),
                pltpu.SemaphoreType.DMA((order // 8,)),
            ],
            compiler_params=pltpu.CompilerParams(vmem_limit_bytes=48 * 1024 * 1024),
            name="fit",
        )(total.reshape(n * rows, snaps), pairs, weights)

    in_specs = (P(("gx", "gy"), None), P(("gx", "gy"), None), P(("gx", "gy"), None), P(), P())
    return jax.shard_map(on_device, mesh=mesh, in_specs=in_specs, out_specs=P(), check_vma=False)
```

```python
import functools
import math

import jax
import jax.numpy as jnp
from jax import lax
from jax.experimental import pallas as pl
from jax.experimental.pallas import tpu as pltpu
from jax.sharding import PartitionSpec as P

MESH = pl.DeviceIdType.MESH
LANES = 128
TILE = 256
CHUNK = 1536
highest = lax.Precision.HIGHEST
VM = pl.BlockSpec(memory_space=pltpu.VMEM)


def dot(a, b, ca, cb, precision=None):
    return lax.dot_general(
        a, b, (((ca,), (cb,)), ((), ())), precision=precision, preferred_element_type=jnp.float32
    )


def project_kernel(gx, gy, basis_ref, snap_ref, deriv_ref, pairs_ref, pen_ref,
                   rates_ref, kernel_ref, dhi_ref, dlo_ref, weights_ref,
                   part, near, mine, got, full, index_ref, sems):
    pairs = gx * gy // 2
    flat = lax.axis_index("gx") * gy + lax.axis_index("gy")
    side, spot = lax.rem(flat, 2), flat // 2
    order = basis_ref.shape[0]
    count = pairs_ref.shape[1]
    padded = dhi_ref.shape[1]

    def device(number):
        return (number // gy, lax.rem(number, gy))

    def other(k):
        return lax.rem(spot + k, pairs)

    mate = device(flat + 1 - 2 * side)
    barrier = pltpu.get_barrier_semaphore()

    def greet(k, c):
        pl.semaphore_signal(barrier, inc=1, device_id=device(other(k) * 2 + side), device_id_type=MESH)
        return c

    pl.semaphore_signal(barrier, inc=1, device_id=mate, device_id_type=MESH)
    lax.fori_loop(1, pairs, greet, 0)

    def remote(src, dst, which, phase, k, at):
        return pltpu.make_async_remote_copy(
            src_ref=src, dst_ref=dst, send_sem=sems.at[which, phase, 0, k],
            recv_sem=sems.at[which, phase, 1, k], device_id=at, device_id_type=MESH)

    def swap(c):
        return remote(part.at[c, 1 - side], near.at[c], c, 0, 0, mate)

    def scatter(c, k):
        to = other(k)
        return remote(mine.at[c, to], got.at[c, spot], c, 1, k, device(to * 2 + side))

    def spread(c, k):
        here = full.at[c, side, spot]
        return remote(here, here, c, 2, k, device(other(k) * 2 + side))

    def relay(c):
        here = full.at[c, side]
        return remote(here, here, c, 3, 0, mate)

    def each(make, c, act):
        def go(k, carry):
            getattr(make(c, k), act)()
            return carry
        lax.fori_loop(1, pairs, go, 0)

    basis = basis_ref[...]

    def project(c, ref):
        prod = dot(basis, ref[...], 1, 0)
        prod = jnp.concatenate([prod, jnp.zeros((LANES - order, prod.shape[1]), jnp.float32)], axis=0)
        for h in range(2):
            part[c, h] = prod[:, h * LANES:(h + 1) * LANES].reshape(part.shape[2:])

    def share(c):
        swap(c).wait()
        total = part[c, side] + near[c]
        mine[c] = total
        each(scatter, c, "start")
        got[c, spot] = mine[c, spot]

    def collect(c):
        each(scatter, c, "wait")
        full[c, side, spot] = jnp.sum(got[c], axis=0)
        each(spread, c, "start")

    def whole(c):
        return jnp.concatenate([full[c, h].reshape(LANES, LANES) for h in range(2)], axis=1)

    project(0, snap_ref)
    pl.semaphore_wait(barrier, pairs)
    swap(0).start()
    project(1, deriv_ref)
    swap(1).start()
    share(0)
    share(1)

    linear = lax.broadcasted_iota(jnp.int32, (2, 1 + order), 1) - 1
    fixed = jnp.where((lax.broadcasted_iota(jnp.int32, (2, 1 + order), 0) == 0) & (linear >= 0), linear, order)
    tail = jnp.full((2, padded - 1 - order - count), LANES - 1, jnp.int32)
    index_ref[...] = jnp.concatenate([fixed, pairs_ref[...], tail], axis=1)
    weights_ref[...] = jnp.zeros_like(weights_ref)
    weights_ref[0:1, 0:1 + order + count] = pen_ref[...][None, :]

    collect(0)
    collect(1)
    each(spread, 0, "wait")
    relay(0).start()
    relay(0).wait()
    coeffs = whole(0)
    ct = coeffs.T
    table = jnp.where(lax.broadcasted_iota(jnp.int32, ct.shape, 1) == order, 1.0, ct)
    t_hi = table.astype(jnp.bfloat16)
    table2 = jnp.concatenate([t_hi, (table - t_hi.astype(jnp.float32)).astype(jnp.bfloat16)], axis=1)
    io = lax.broadcasted_iota(jnp.int32, (LANES, TILE), 0)
    each(spread, 1, "wait")
    relay(1).start()

    def pick_mxu(row):
        hot = jnp.where(io == row, 1.0, 0.0).astype(jnp.bfloat16)
        return dot(table2, jnp.concatenate([hot, hot], axis=0), 1, 0)

    def pick_xlu(row):
        return jnp.concatenate([jnp.take_along_axis(
            table, jnp.broadcast_to(row[:, h:h + LANES], table.shape), axis=1, mode="promise_in_bounds")
            for h in range(0, TILE, LANES)], axis=1)

    def build(at, carry):
        for u in range(CHUNK // TILE):
            sl = pl.ds(pl.multiple_of(at * CHUNK + u * TILE, TILE), TILE)
            d = pick_xlu(index_ref[0:1, sl]) * pick_mxu(index_ref[1:2, sl])
            d_hi = d.astype(jnp.bfloat16)
            dhi_ref[:, sl] = d_hi
            dlo_ref[:, sl] = (d - d_hi.astype(jnp.float32)).astype(jnp.bfloat16)
        return carry

    lax.fori_loop(0, padded // CHUNK, build, 0)
    inner = dot(ct, coeffs, 1, 0, highest)
    sq = coeffs * coeffs
    kernel_ref[...] = 1.0 + inner + 0.5 * (inner * inner + dot(ct * ct, sq, 1, 0, highest))
    relay(1).wait()
    rates_ref[...] = whole(1)[:order]


def fit_kernel(rates_ref, kernel_ref, dhi_ref, dlo_ref, pen_ref, out_ref, t_ref, w_ref, x_ref, pt_ref, sem):
    order, snaps = rates_ref.shape
    padded = t_ref.shape[1]
    width = x_ref.shape[1]
    g = rates_ref[...] * (1.0 / math.sqrt(snaps))
    kernel = kernel_ref[...]
    s1 = dot(g, kernel, 1, 0, highest)
    lhs = jnp.concatenate([g, s1 * (1.0 / snaps)], axis=0)
    lhs_hi = lhs.astype(jnp.bfloat16)
    lhs_lo = (lhs - lhs_hi.astype(jnp.float32)).astype(jnp.bfloat16)
    lhs_both = jnp.concatenate([lhs_hi, lhs_lo], axis=0)

    def tile(at, carry):
        tt, tw = carry
        for u in range(CHUNK // TILE):
            sl = pl.ds(pl.multiple_of(at * CHUNK + u * TILE, TILE), TILE)
            both = dot(lhs_both, dhi_ref[:, sl], 1, 0)
            tv = both[:2 * order] + both[2 * order:] + dot(lhs_hi, dlo_ref[:, sl], 1, 0)
            t, v = tv[:order], tv[order:]
            pt = pen_ref[0:1, sl] * t
            w = v + pt
            t_ref[:, sl] = t
            w_ref[:, sl] = w
            pt_ref[:, sl] = pt.astype(jnp.bfloat16)
            sq, cross = t * t, t * w
            for h in range(0, TILE, LANES):
                tt = tt + sq[:, h:h + LANES]
                tw = tw + cross[:, h:h + LANES]
        return tt, tw

    zero = jnp.zeros((order, LANES), jnp.float32)
    tt, tw = lax.fori_loop(0, padded // CHUNK, tile, (zero, zero))
    dpt = dot(dhi_ref[...], pt_ref[...], 1, 1)
    tt = jnp.sum(tt, axis=1, keepdims=True)
    tw = jnp.sum(tw, axis=1, keepdims=True)
    alpha = tt / tw
    ks1 = dot(s1, kernel, 1, 0, highest) * (1.0 / snaps)
    image = ks1 + jnp.pad(dpt, ((0, 0), (0, LANES - order))).T[:order]
    moved = s1 - alpha * image
    gram = jnp.sum(moved * moved, axis=1, keepdims=True) * (1.0 / snaps)
    group = 8 * max(d for d in range(1, 6) if order // 8 % d == 0)
    copies = []
    for at in range(0, order, group):
        rows = slice(at, at + group)
        a = alpha[rows]
        t, w = t_ref[rows, :], w_ref[rows, :]
        r = t - a * w
        rr = r * r
        weighted = jnp.sum(rr * pen_ref[0:1, :], axis=1, keepdims=True) + gram[rows]
        now = jnp.sum(rr, axis=1, keepdims=True)
        ratio = now / tt[rows]
        second = now / (weighted - ratio * now / a)
        x = (a + second * ratio) * t + second * r
        x_ref[rows, :] = x[:, :width]
        copy = pltpu.make_async_copy(x_ref.at[rows, :], out_ref.at[rows, :], sem.at[at // group])
        copy.start()
        copies.append(copy)
    for copy in copies:
        copy.wait()


def solution(mesh):
    gx, gy = mesh.shape["gx"], mesh.shape["gy"]
    pairs = gx * gy // 2

    def on_device(basis, snapshots, derivatives, quad_pairs, penalty):
        order, snaps = basis.shape[1], snapshots.shape[1]
        width = 1 + order + quad_pairs.shape[1]
        padded = -(-width // CHUNK) * CHUNK
        f32, bf16 = jnp.float32, jnp.bfloat16
        block = (pairs, LANES // pairs, LANES)
        rates, kernel, dhi, dlo, weights = pl.pallas_call(
            functools.partial(project_kernel, gx, gy),
            out_shape=[
                jax.ShapeDtypeStruct((order, snaps), f32),
                jax.ShapeDtypeStruct((snaps, snaps), f32),
                jax.ShapeDtypeStruct((snaps, padded), bf16),
                jax.ShapeDtypeStruct((snaps, padded), bf16),
                jax.ShapeDtypeStruct((1, padded), f32),
            ],
            in_specs=[VM] * 5,
            out_specs=[VM] * 5,
            scratch_shapes=[
                pltpu.VMEM((2, 2) + block, f32),
                pltpu.VMEM((2,) + block, f32),
                pltpu.VMEM((2,) + block, f32),
                pltpu.VMEM((2,) + block, f32),
                pltpu.VMEM((2, 2) + block, f32),
                pltpu.VMEM((2, padded), jnp.int32),
                pltpu.SemaphoreType.DMA((2, 4, 2, pairs)),
            ],
            compiler_params=pltpu.CompilerParams(
                collective_id=0, has_side_effects=True, vmem_limit_bytes=24 * 1024 * 1024),
            name="project",
        )(basis.T, snapshots, derivatives, quad_pairs, penalty)
        return pl.pallas_call(
            fit_kernel,
            out_shape=jax.ShapeDtypeStruct((order, width), f32),
            in_specs=[VM] * 5,
            out_specs=pl.BlockSpec(memory_space=pl.ANY),
            scratch_shapes=[
                pltpu.VMEM((order, padded), f32),
                pltpu.VMEM((order, padded), f32),
                pltpu.VMEM((order, width), f32),
                pltpu.VMEM((order, padded), bf16),
                pltpu.SemaphoreType.DMA((order // 8,)),
            ],
            compiler_params=pltpu.CompilerParams(vmem_limit_bytes=24 * 1024 * 1024),
            name="fit",
        )(rates, kernel, dhi, dlo, weights)

    in_specs = (P(("gx", "gy"), None), P(("gx", "gy"), None), P(("gx", "gy"), None), P(), P())
    return jax.shard_map(on_device, mesh=mesh, in_specs=in_specs, out_specs=P(), check_vma=False)
```

```python
import functools
import math

import jax
import jax.numpy as jnp
from jax import lax
from jax.experimental import pallas as pl
from jax.experimental.pallas import tpu as pltpu
from jax.sharding import PartitionSpec as P

MESH = pl.DeviceIdType.MESH
LANES = 128
TILE = 256
CHUNK = 1536
highest = lax.Precision.HIGHEST
VM = pl.BlockSpec(memory_space=pltpu.VMEM)
HBM = pl.BlockSpec(memory_space=pltpu.HBM)


def dot(a, b, ca, cb, precision=None):
    return lax.dot_general(
        a, b, (((ca,), (cb,)), ((), ())), precision=precision, preferred_element_type=jnp.float32
    )


def project_kernel(gx, gy, basis_hbm, snap_hbm, deriv_hbm, pairs_hbm, pen_hbm,
                   rates_ref, kernel_ref, dhi_ref, dlo_ref, weights_ref,
                   basis_ref, snap_ref, deriv_ref, pairs_ref, pen_ref,
                   part, near, mine, got, full, hot_i, hot_j, load_sems, sems):
    pairs = gx * gy // 2
    flat = lax.axis_index("gx") * gy + lax.axis_index("gy")
    side, spot = lax.rem(flat, 2), flat // 2
    order = basis_ref.shape[0]
    count = pairs_ref.shape[1]
    padded = dhi_ref.shape[1]

    def device(number):
        return (number // gy, lax.rem(number, gy))

    def other(k):
        return lax.rem(spot + k, pairs)

    mate = device(flat + 1 - 2 * side)
    barrier = pltpu.get_barrier_semaphore()

    def greet(k, c):
        pl.semaphore_signal(barrier, inc=1, device_id=device(other(k) * 2 + side), device_id_type=MESH)
        return c

    pl.semaphore_signal(barrier, inc=1, device_id=mate, device_id_type=MESH)
    lax.fori_loop(1, pairs, greet, 0)
    loads = [
        pltpu.make_async_copy(src, dst, load_sems.at[k])
        for k, (src, dst) in enumerate((
            (basis_hbm, basis_ref), (snap_hbm, snap_ref), (deriv_hbm, deriv_ref),
            (pairs_hbm, pairs_ref), (pen_hbm, pen_ref)))
    ]
    for load in loads:
        load.start()

    def remote(src, dst, which, phase, k, at):
        return pltpu.make_async_remote_copy(
            src_ref=src, dst_ref=dst, send_sem=sems.at[which, phase, 0, k],
            recv_sem=sems.at[which, phase, 1, k], device_id=at, device_id_type=MESH)

    def swap(c):
        return remote(part.at[c, 1 - side], near.at[c], c, 0, 0, mate)

    def scatter(c, k):
        to = other(k)
        return remote(mine.at[c, to], got.at[c, spot], c, 1, k, device(to * 2 + side))

    def spread(c, k):
        here = full.at[c, side, spot]
        return remote(here, here, c, 2, k, device(other(k) * 2 + side))

    def relay(c):
        here = full.at[c, side]
        return remote(here, here, c, 3, 0, mate)

    def each(make, c, act):
        def go(k, carry):
            getattr(make(c, k), act)()
            return carry
        lax.fori_loop(1, pairs, go, 0)

    def project(c, ref):
        prod = dot(basis_ref[...], ref[...], 1, 0)
        prod = jnp.concatenate([prod, jnp.zeros((LANES - order, prod.shape[1]), jnp.float32)], axis=0)
        for h in range(2):
            part[c, h] = prod[:, h * LANES:(h + 1) * LANES].reshape(part.shape[2:])

    def share(c):
        swap(c).wait()
        total = part[c, side] + near[c]
        mine[c] = total
        each(scatter, c, "start")
        got[c, spot] = mine[c, spot]

    def collect(c):
        each(scatter, c, "wait")
        full[c, side, spot] = jnp.sum(got[c], axis=0)
        each(spread, c, "start")

    def whole(c):
        return jnp.concatenate([full[c, h].reshape(LANES, LANES) for h in range(2)], axis=1)

    loads[0].wait()
    loads[1].wait()
    project(0, snap_ref)
    pl.semaphore_wait(barrier, pairs)
    swap(0).start()
    loads[2].wait()
    project(1, deriv_ref)
    swap(1).start()
    share(0)
    share(1)

    loads[3].wait()
    loads[4].wait()
    linear = lax.broadcasted_iota(jnp.int32, (2, 1 + order), 1) - 1
    fixed = jnp.where((lax.broadcasted_iota(jnp.int32, (2, 1 + order), 0) == 0) & (linear >= 0), linear, order)
    tail = jnp.full((2, padded - 1 - order - count), LANES - 1, jnp.int32)
    index = jnp.concatenate([fixed, pairs_ref[...], tail], axis=1)
    io = lax.broadcasted_iota(jnp.int32, (LANES, padded), 0)
    hot_i[...] = jnp.where(io == index[0:1], 1.0, 0.0).astype(jnp.bfloat16)
    hot_j[...] = jnp.where(io == index[1:2], 1.0, 0.0).astype(jnp.bfloat16)
    weights_ref[...] = jnp.zeros_like(weights_ref)
    weights_ref[0:1, 0:1 + order + count] = pen_ref[...][None, :]

    def build(h):
        table = full[0, h].reshape(LANES, LANES).T
        table = jnp.where(lax.broadcasted_iota(jnp.int32, table.shape, 1) == order, 1.0, table)
        t_hi = table.astype(jnp.bfloat16)
        both = jnp.concatenate([t_hi, (table - t_hi.astype(jnp.float32)).astype(jnp.bfloat16)], axis=1)
        rows = pl.ds(pl.multiple_of(h * LANES, LANES), LANES)

        def pick(ref, sl):
            hot = ref[:, sl]
            return dot(both, jnp.concatenate([hot, hot], axis=0), 1, 0)

        def step(at, carry):
            for u in range(CHUNK // TILE):
                sl = pl.ds(pl.multiple_of(at * CHUNK + u * TILE, TILE), TILE)
                d = pick(hot_i, sl) * pick(hot_j, sl)
                d_hi = d.astype(jnp.bfloat16)
                dhi_ref[rows, sl] = d_hi
                dlo_ref[rows, sl] = (d - d_hi.astype(jnp.float32)).astype(jnp.bfloat16)
            return carry

        lax.fori_loop(0, padded // CHUNK, step, 0)

    collect(0)
    collect(1)
    each(spread, 0, "wait")
    relay(0).start()
    build(side)
    relay(0).wait()
    each(spread, 1, "wait")
    relay(1).start()
    build(1 - side)
    coeffs = whole(0)
    ct = coeffs.T
    inner = dot(ct, coeffs, 1, 0, highest)
    sq = coeffs * coeffs
    kernel_ref[...] = 1.0 + inner + 0.5 * (inner * inner + dot(ct * ct, sq, 1, 0, highest))
    relay(1).wait()
    rates_ref[...] = whole(1)[:order]


def fit_kernel(rates_ref, kernel_ref, dhi_ref, dlo_ref, pen_ref, out_ref, t_ref, w_ref, x_ref, pt_ref, sem):
    order, snaps = rates_ref.shape
    padded = t_ref.shape[1]
    width = x_ref.shape[1]
    g = rates_ref[...] * (1.0 / math.sqrt(snaps))
    kernel = kernel_ref[...]
    s1 = dot(g, kernel, 1, 0, highest)
    lhs = jnp.concatenate([g, s1 * (1.0 / snaps)], axis=0)
    lhs_hi = lhs.astype(jnp.bfloat16)
    lhs_lo = (lhs - lhs_hi.astype(jnp.float32)).astype(jnp.bfloat16)
    lhs_both = jnp.concatenate([lhs_hi, lhs_lo], axis=0)

    def tile(at, carry):
        tt, tw = carry
        for u in range(CHUNK // TILE):
            sl = pl.ds(pl.multiple_of(at * CHUNK + u * TILE, TILE), TILE)
            both = dot(lhs_both, dhi_ref[:, sl], 1, 0)
            tv = both[:2 * order] + both[2 * order:] + dot(lhs_hi, dlo_ref[:, sl], 1, 0)
            t, v = tv[:order], tv[order:]
            pt = pen_ref[0:1, sl] * t
            w = v + pt
            t_ref[:, sl] = t
            w_ref[:, sl] = w
            pt_ref[:, sl] = pt.astype(jnp.bfloat16)
            sq, cross = t * t, t * w
            for h in range(0, TILE, LANES):
                tt = tt + sq[:, h:h + LANES]
                tw = tw + cross[:, h:h + LANES]
        return tt, tw

    zero = jnp.zeros((order, LANES), jnp.float32)
    tt, tw = lax.fori_loop(0, padded // CHUNK, tile, (zero, zero))
    dpt = dot(dhi_ref[...], pt_ref[...], 1, 1)
    tt = jnp.sum(tt, axis=1, keepdims=True)
    tw = jnp.sum(tw, axis=1, keepdims=True)
    alpha = tt / tw
    ks1 = dot(s1, kernel, 1, 0, highest) * (1.0 / snaps)
    image = ks1 + jnp.pad(dpt, ((0, 0), (0, LANES - order))).T[:order]
    moved = s1 - alpha * image
    gram = jnp.sum(moved * moved, axis=1, keepdims=True) * (1.0 / snaps)
    group = 8 * max(d for d in range(1, 6) if order // 8 % d == 0)
    copies = []
    for at in range(0, order, group):
        rows = slice(at, at + group)
        a = alpha[rows]
        t, w = t_ref[rows, :], w_ref[rows, :]
        r = t - a * w
        rr = r * r
        weighted = jnp.sum(rr * pen_ref[0:1, :], axis=1, keepdims=True) + gram[rows]
        now = jnp.sum(rr, axis=1, keepdims=True)
        ratio = now / tt[rows]
        second = now / (weighted - ratio * now / a)
        x = (a + second * ratio) * t + second * r
        x_ref[rows, :] = x[:, :width]
        copy = pltpu.make_async_copy(x_ref.at[rows, :], out_ref.at[rows, :], sem.at[at // group])
        copy.start()
        copies.append(copy)
    for copy in copies:
        copy.wait()


def solution(mesh):
    gx, gy = mesh.shape["gx"], mesh.shape["gy"]
    pairs = gx * gy // 2

    def on_device(basis, snapshots, derivatives, quad_pairs, penalty):
        order, snaps = basis.shape[1], snapshots.shape[1]
        width = 1 + order + quad_pairs.shape[1]
        padded = -(-width // CHUNK) * CHUNK
        f32, bf16 = jnp.float32, jnp.bfloat16
        block = (pairs, LANES // pairs, LANES)
        rates, kernel, dhi, dlo, weights = pl.pallas_call(
            functools.partial(project_kernel, gx, gy),
            out_shape=[
                jax.ShapeDtypeStruct((order, snaps), f32),
                jax.ShapeDtypeStruct((snaps, snaps), f32),
                jax.ShapeDtypeStruct((snaps, padded), bf16),
                jax.ShapeDtypeStruct((snaps, padded), bf16),
                jax.ShapeDtypeStruct((1, padded), f32),
            ],
            in_specs=[HBM] * 5,
            out_specs=[VM] * 5,
            scratch_shapes=[
                pltpu.VMEM((order, basis.shape[0]), bf16),
                pltpu.VMEM(snapshots.shape, bf16),
                pltpu.VMEM(derivatives.shape, bf16),
                pltpu.VMEM(quad_pairs.shape, jnp.int32),
                pltpu.VMEM(penalty.shape, f32),
                pltpu.VMEM((2, 2) + block, f32),
                pltpu.VMEM((2,) + block, f32),
                pltpu.VMEM((2,) + block, f32),
                pltpu.VMEM((2,) + block, f32),
                pltpu.VMEM((2, 2) + block, f32),
                pltpu.VMEM((LANES, padded), bf16),
                pltpu.VMEM((LANES, padded), bf16),
                pltpu.SemaphoreType.DMA((5,)),
                pltpu.SemaphoreType.DMA((2, 4, 2, pairs)),
            ],
            compiler_params=pltpu.CompilerParams(
                collective_id=0, has_side_effects=True, vmem_limit_bytes=24 * 1024 * 1024),
            name="project",
        )(*(pltpu.with_memory_space_constraint(v, pltpu.HBM) for v in (basis.T, snapshots, derivatives, quad_pairs, penalty)))
        return pl.pallas_call(
            fit_kernel,
            out_shape=jax.ShapeDtypeStruct((order, width), f32),
            in_specs=[VM] * 5,
            out_specs=pl.BlockSpec(memory_space=pl.ANY),
            scratch_shapes=[
                pltpu.VMEM((order, padded), f32),
                pltpu.VMEM((order, padded), f32),
                pltpu.VMEM((order, width), f32),
                pltpu.VMEM((order, padded), bf16),
                pltpu.SemaphoreType.DMA((order // 8,)),
            ],
            compiler_params=pltpu.CompilerParams(vmem_limit_bytes=24 * 1024 * 1024),
            name="fit",
        )(rates, kernel, dhi, dlo, weights)

    in_specs = (P(("gx", "gy"), None), P(("gx", "gy"), None), P(("gx", "gy"), None), P(), P())
    return jax.shard_map(on_device, mesh=mesh, in_specs=in_specs, out_specs=P(), check_vma=False)
```

```python
import functools
import math

import jax
import jax.numpy as jnp
from jax import lax
from jax.experimental import pallas as pl
from jax.experimental.pallas import tpu as pltpu
from jax.sharding import PartitionSpec as P

MESH = pl.DeviceIdType.MESH
LANES = 128
TILE = 256
CHUNK = 3840
highest = lax.Precision.HIGH
VM = pl.BlockSpec(memory_space=pltpu.VMEM)
HBM = pl.BlockSpec(memory_space=pltpu.HBM)


def dot(a, b, ca, cb, precision=None):
    return lax.dot_general(
        a, b, (((ca,), (cb,)), ((), ())), precision=precision, preferred_element_type=jnp.float32
    )


def project_kernel(gx, gy, basis_hbm, snap_hbm, deriv_hbm, pairs_hbm, pen_hbm,
                   rates_ref, kernel_ref, dhi_ref, dlo_ref, weights_ref,
                   basis_ref, snap_ref, deriv_ref, pairs_ref, pen_ref,
                   part, near, mine, got, full, hot_i, hot_j, load_sems, sems):
    pairs = gx * gy // 2
    flat = lax.axis_index("gx") * gy + lax.axis_index("gy")
    side, spot = lax.rem(flat, 2), flat // 2
    order = basis_ref.shape[0]
    count = pairs_ref.shape[1]
    padded = dhi_ref.shape[1]

    def device(number):
        return (number // gy, lax.rem(number, gy))

    def other(k):
        return lax.rem(spot + k, pairs)

    mate = device(flat + 1 - 2 * side)
    barrier = pltpu.get_barrier_semaphore()

    def greet(k, c):
        pl.semaphore_signal(barrier, inc=1, device_id=device(other(k) * 2 + side), device_id_type=MESH)
        return c

    pl.semaphore_signal(barrier, inc=1, device_id=mate, device_id_type=MESH)
    lax.fori_loop(1, pairs, greet, 0)
    loads = [
        pltpu.make_async_copy(src, dst, load_sems.at[k])
        for k, (src, dst) in enumerate((
            (basis_hbm, basis_ref), (snap_hbm, snap_ref), (deriv_hbm, deriv_ref),
            (pairs_hbm, pairs_ref), (pen_hbm, pen_ref)))
    ]
    for load in loads:
        load.start()

    def remote(src, dst, which, phase, k, at):
        return pltpu.make_async_remote_copy(
            src_ref=src, dst_ref=dst, send_sem=sems.at[which, phase, 0, k],
            recv_sem=sems.at[which, phase, 1, k], device_id=at, device_id_type=MESH)

    def swap(c):
        return remote(part.at[c, 1 - side], near.at[c], c, 0, 0, mate)

    def scatter(c, k):
        to = other(k)
        return remote(mine.at[c, to], got.at[c, spot], c, 1, k, device(to * 2 + side))

    def spread(c, k):
        here = full.at[c, side, spot]
        return remote(here, here, c, 2, k, device(other(k) * 2 + side))

    def relay(c):
        here = full.at[c, side]
        return remote(here, here, c, 3, 0, mate)

    upper = spot // (pairs // 2)

    def each(make, c, act):
        def go(j, carry):
            k = upper * j + (1 - upper) * (pairs - j)
            getattr(make(c, k), act)()
            return carry
        lax.fori_loop(1, pairs, go, 0)

    def project(c, ref):
        prod = dot(basis_ref[...], ref[...], 1, 0)
        prod = jnp.concatenate([prod, jnp.zeros((LANES - order, prod.shape[1]), jnp.float32)], axis=0)
        for h in range(2):
            part[c, h] = prod[:, h * LANES:(h + 1) * LANES].reshape(part.shape[2:])

    def share(c):
        swap(c).wait()
        total = part[c, side] + near[c]
        mine[c] = total
        each(scatter, c, "start")
        got[c, spot] = mine[c, spot]

    def collect(c):
        each(scatter, c, "wait")
        full[c, side, spot] = jnp.sum(got[c], axis=0)
        each(spread, c, "start")

    def whole(c):
        return jnp.concatenate([full[c, h].reshape(LANES, LANES) for h in range(2)], axis=1)

    loads[0].wait()
    loads[1].wait()
    project(0, snap_ref)
    pl.semaphore_wait(barrier, pairs)
    swap(0).start()
    loads[2].wait()
    project(1, deriv_ref)
    swap(1).start()
    share(0)
    share(1)

    loads[3].wait()
    loads[4].wait()
    linear = lax.broadcasted_iota(jnp.int32, (2, 1 + order), 1) - 1
    fixed = jnp.where((lax.broadcasted_iota(jnp.int32, (2, 1 + order), 0) == 0) & (linear >= 0), linear, order)
    tail = jnp.full((2, padded - 1 - order - count), LANES - 1, jnp.int32)
    index = jnp.concatenate([fixed, pairs_ref[...], tail], axis=1)
    io = lax.broadcasted_iota(jnp.int32, (LANES, padded), 0)
    hot_i[...] = jnp.where(io == index[0:1], 1.0, 0.0).astype(jnp.bfloat16)
    hot_j[...] = jnp.where(io == index[1:2], 1.0, 0.0).astype(jnp.bfloat16)
    weights_ref[...] = jnp.zeros_like(weights_ref)
    weights_ref[0:1, 0:1 + order + count] = pen_ref[...][None, :]

    def build(h):
        table = full[0, h].reshape(LANES, LANES).T
        table = jnp.where(lax.broadcasted_iota(jnp.int32, table.shape, 1) == order, 1.0, table)
        t_hi = table.astype(jnp.bfloat16)
        both = jnp.concatenate([t_hi, (table - t_hi.astype(jnp.float32)).astype(jnp.bfloat16)], axis=1)
        rows = pl.ds(pl.multiple_of(h * LANES, LANES), LANES)

        def pick(ref, sl):
            hot = ref[:, sl]
            return dot(both, jnp.concatenate([hot, hot], axis=0), 1, 0)

        def step(at, carry):
            for u in range(CHUNK // TILE):
                sl = pl.ds(pl.multiple_of(at * CHUNK + u * TILE, TILE), TILE)
                d = pick(hot_i, sl) * pick(hot_j, sl)
                d_hi = d.astype(jnp.bfloat16)
                dhi_ref[rows, sl] = d_hi
                dlo_ref[rows, sl] = (d - d_hi.astype(jnp.float32)).astype(jnp.bfloat16)
            return carry

        lax.fori_loop(0, padded // CHUNK, step, 0)

    collect(0)
    collect(1)
    each(spread, 0, "wait")
    relay(0).start()
    build(side)
    relay(0).wait()
    each(spread, 1, "wait")
    relay(1).start()
    build(1 - side)
    coeffs = whole(0)
    ct = coeffs.T
    inner = dot(ct, coeffs, 1, 0, highest)
    sq = coeffs * coeffs
    kernel_ref[...] = 1.0 + inner + 0.5 * (inner * inner + dot(ct * ct, sq, 1, 0, highest))
    relay(1).wait()
    rates_ref[...] = whole(1)[:order]


def fit_kernel(rates_ref, kernel_ref, dhi_ref, dlo_ref, pen_ref, out_ref, t_ref, w_ref, x_ref, pt_ref, sem):
    order, snaps = rates_ref.shape
    padded = t_ref.shape[1]
    width = x_ref.shape[1]
    g = rates_ref[...] * (1.0 / math.sqrt(snaps))
    kernel = kernel_ref[...]
    s1 = dot(g, kernel, 1, 0, highest)
    lhs = jnp.concatenate([g, s1 * (1.0 / snaps)], axis=0)
    lhs_hi = lhs.astype(jnp.bfloat16)
    lhs_lo = (lhs - lhs_hi.astype(jnp.float32)).astype(jnp.bfloat16)
    lhs_both = jnp.concatenate([lhs_hi, lhs_lo], axis=0)

    def tile(at, carry):
        tt, tw = carry
        for u in range(CHUNK // TILE):
            sl = pl.ds(pl.multiple_of(at * CHUNK + u * TILE, TILE), TILE)
            both = dot(lhs_both, dhi_ref[:, sl], 1, 0)
            tv = both[:2 * order] + both[2 * order:] + dot(lhs_hi, dlo_ref[:, sl], 1, 0)
            t, v = tv[:order], tv[order:]
            pt = pen_ref[0:1, sl] * t
            w = v + pt
            t_ref[:, sl] = t
            w_ref[:, sl] = w
            pt_ref[:, sl] = pt.astype(jnp.bfloat16)
            sq, cross = t * t, t * w
            for h in range(0, TILE, LANES):
                tt = tt + sq[:, h:h + LANES]
                tw = tw + cross[:, h:h + LANES]
        return tt, tw

    zero = jnp.zeros((order, LANES), jnp.float32)
    tt, tw = lax.fori_loop(0, padded // CHUNK, tile, (zero, zero))
    dpt = dot(dhi_ref[...], pt_ref[...], 1, 1)
    tt = jnp.sum(tt, axis=1, keepdims=True)
    tw = jnp.sum(tw, axis=1, keepdims=True)
    alpha = tt / tw
    ks1 = dot(s1, kernel, 1, 0, highest) * (1.0 / snaps)
    image = ks1 + jnp.pad(dpt, ((0, 0), (0, LANES - order))).T[:order]
    moved = s1 - alpha * image
    gram = jnp.sum(moved * moved, axis=1, keepdims=True) * (1.0 / snaps)
    group = 8 * max(d for d in range(1, 4) if order // 8 % d == 0)
    copies = []
    for at in range(0, order, group):
        rows = slice(at, at + group)
        a = alpha[rows]
        t, w = t_ref[rows, :], w_ref[rows, :]
        r = t - a * w
        rr = r * r
        weighted = jnp.sum(rr * pen_ref[0:1, :], axis=1, keepdims=True) + gram[rows]
        now = jnp.sum(rr, axis=1, keepdims=True)
        ratio = now / tt[rows]
        second = now / (weighted - ratio * now / a)
        x = (a + second * ratio + second) * t - (second * a) * w
        x_ref[rows, :] = x[:, :width]
        copy = pltpu.make_async_copy(x_ref.at[rows, :], out_ref.at[rows, :], sem.at[at // group])
        copy.start()
        copies.append(copy)
    for copy in copies:
        copy.wait()


def solution(mesh):
    gx, gy = mesh.shape["gx"], mesh.shape["gy"]
    pairs = gx * gy // 2

    def on_device(basis, snapshots, derivatives, quad_pairs, penalty):
        order, snaps = basis.shape[1], snapshots.shape[1]
        width = 1 + order + quad_pairs.shape[1]
        padded = -(-width // CHUNK) * CHUNK
        f32, bf16 = jnp.float32, jnp.bfloat16
        block = (pairs, LANES // pairs, LANES)
        rates, kernel, dhi, dlo, weights = pl.pallas_call(
            functools.partial(project_kernel, gx, gy),
            out_shape=[
                jax.ShapeDtypeStruct((order, snaps), f32),
                jax.ShapeDtypeStruct((snaps, snaps), f32),
                jax.ShapeDtypeStruct((snaps, padded), bf16),
                jax.ShapeDtypeStruct((snaps, padded), bf16),
                jax.ShapeDtypeStruct((1, padded), f32),
            ],
            in_specs=[HBM] * 5,
            out_specs=[VM] * 5,
            scratch_shapes=[
                pltpu.VMEM((order, basis.shape[0]), bf16),
                pltpu.VMEM(snapshots.shape, bf16),
                pltpu.VMEM(derivatives.shape, bf16),
                pltpu.VMEM(quad_pairs.shape, jnp.int32),
                pltpu.VMEM(penalty.shape, f32),
                pltpu.VMEM((2, 2) + block, f32),
                pltpu.VMEM((2,) + block, f32),
                pltpu.VMEM((2,) + block, f32),
                pltpu.VMEM((2,) + block, f32),
                pltpu.VMEM((2, 2) + block, f32),
                pltpu.VMEM((LANES, padded), bf16),
                pltpu.VMEM((LANES, padded), bf16),
                pltpu.SemaphoreType.DMA((5,)),
                pltpu.SemaphoreType.DMA((2, 4, 2, pairs)),
            ],
            compiler_params=pltpu.CompilerParams(
                collective_id=0, has_side_effects=True, vmem_limit_bytes=24 * 1024 * 1024),
            name="project",
        )(*(pltpu.with_memory_space_constraint(v, pltpu.HBM) for v in (basis.T, snapshots, derivatives, quad_pairs, penalty)))
        return pl.pallas_call(
            fit_kernel,
            out_shape=jax.ShapeDtypeStruct((order, width), f32),
            in_specs=[VM] * 5,
            out_specs=pl.BlockSpec(memory_space=pl.ANY),
            scratch_shapes=[
                pltpu.VMEM((order, padded), f32),
                pltpu.VMEM((order, padded), f32),
                pltpu.VMEM((order, width), f32),
                pltpu.VMEM((order, padded), bf16),
                pltpu.SemaphoreType.DMA((order // 8,)),
            ],
            compiler_params=pltpu.CompilerParams(vmem_limit_bytes=24 * 1024 * 1024),
            name="fit",
        )(rates, kernel, dhi, dlo, weights)

    in_specs = (P(("gx", "gy"), None), P(("gx", "gy"), None), P(("gx", "gy"), None), P(), P())
    return jax.shard_map(on_device, mesh=mesh, in_specs=in_specs, out_specs=P(), check_vma=False)
```

```python
import functools
import math

import jax
import jax.numpy as jnp
from jax import lax
from jax.experimental import pallas as pl
from jax.experimental.pallas import tpu as pltpu
from jax.sharding import PartitionSpec as P

MESH = pl.DeviceIdType.MESH
LANES = 128
TILE = 256
CHUNK = 7680
highest = lax.Precision.HIGH
VM = pl.BlockSpec(memory_space=pltpu.VMEM)
HBM = pl.BlockSpec(memory_space=pltpu.HBM)


def dot(a, b, ca, cb, precision=None):
    return lax.dot_general(
        a, b, (((ca,), (cb,)), ((), ())), precision=precision, preferred_element_type=jnp.float32
    )


def project_kernel(gx, gy, basis_hbm, snap_hbm, deriv_hbm, pairs_hbm, pen_hbm,
                   rates_ref, kernel_ref, dhi_ref, dlo_ref, weights_ref,
                   basis_ref, snap_ref, deriv_ref, pairs_ref, pen_ref,
                   part, near, mine, got, full, hot_i, hot_j, load_sems, sems):
    pairs = gx * gy // 2
    flat = lax.axis_index("gx") * gy + lax.axis_index("gy")
    side, spot = lax.rem(flat, 2), flat // 2
    order = basis_ref.shape[0]
    count = pairs_ref.shape[1]
    padded = dhi_ref.shape[1]

    def device(number):
        return (number // gy, lax.rem(number, gy))

    def other(k):
        return lax.rem(spot + k, pairs)

    mate = device(flat + 1 - 2 * side)
    barrier = pltpu.get_barrier_semaphore()

    def greet(k, c):
        pl.semaphore_signal(barrier, inc=1, device_id=device(other(k) * 2 + side), device_id_type=MESH)
        return c

    pl.semaphore_signal(barrier, inc=1, device_id=mate, device_id_type=MESH)
    lax.fori_loop(1, pairs, greet, 0)
    loads = [
        pltpu.make_async_copy(src, dst, load_sems.at[k])
        for k, (src, dst) in enumerate((
            (basis_hbm, basis_ref), (snap_hbm, snap_ref), (deriv_hbm, deriv_ref),
            (pairs_hbm, pairs_ref), (pen_hbm, pen_ref)))
    ]
    for load in loads:
        load.start()

    def remote(src, dst, which, phase, k, at):
        return pltpu.make_async_remote_copy(
            src_ref=src, dst_ref=dst, send_sem=sems.at[which, phase, 0, k],
            recv_sem=sems.at[which, phase, 1, k], device_id=at, device_id_type=MESH)

    def swap(c):
        return remote(part.at[c, 1 - side], near.at[c], c, 0, 0, mate)

    def scatter(c, k):
        to = other(k)
        return remote(mine.at[c, to], got.at[c, spot], c, 1, k, device(to * 2 + side))

    def spread(c, k):
        here = full.at[c, side, spot]
        return remote(here, here, c, 2, k, device(other(k) * 2 + side))

    def relay(c):
        here = full.at[c, side]
        return remote(here, here, c, 3, 0, mate)

    upper = spot // (pairs // 2)

    def each(make, c, act):
        def go(j, carry):
            k = upper * j + (1 - upper) * (pairs - j)
            getattr(make(c, k), act)()
            return carry
        lax.fori_loop(1, pairs, go, 0)

    def project(c, ref):
        prod = dot(basis_ref[...], ref[...], 1, 0)
        prod = jnp.concatenate([prod, jnp.zeros((LANES - order, prod.shape[1]), jnp.float32)], axis=0)
        for h in range(2):
            part[c, h] = prod[:, h * LANES:(h + 1) * LANES].reshape(part.shape[2:])

    def share(c):
        swap(c).wait()
        total = part[c, side] + near[c]
        mine[c] = total
        each(scatter, c, "start")
        got[c, spot] = mine[c, spot]

    def collect(c):
        each(scatter, c, "wait")
        full[c, side, spot] = jnp.sum(got[c], axis=0)
        each(spread, c, "start")

    def whole(c):
        return jnp.concatenate([full[c, h].reshape(LANES, LANES) for h in range(2)], axis=1)

    loads[0].wait()
    loads[1].wait()
    project(0, snap_ref)
    pl.semaphore_wait(barrier, pairs)
    swap(0).start()
    loads[2].wait()
    project(1, deriv_ref)
    swap(1).start()
    share(0)
    share(1)

    loads[3].wait()
    loads[4].wait()
    linear = lax.broadcasted_iota(jnp.int32, (2, 1 + order), 1) - 1
    fixed = jnp.where((lax.broadcasted_iota(jnp.int32, (2, 1 + order), 0) == 0) & (linear >= 0), linear, order)
    tail = jnp.full((2, padded - 1 - order - count), LANES - 1, jnp.int32)
    index = jnp.concatenate([fixed, pairs_ref[...], tail], axis=1)
    io = lax.broadcasted_iota(jnp.int32, (LANES, padded), 0)
    hot_i[...] = jnp.where(io == index[0:1], 1.0, 0.0).astype(jnp.bfloat16)
    hot_j[...] = jnp.where(io == index[1:2], 1.0, 0.0).astype(jnp.bfloat16)
    weights_ref[...] = jnp.zeros_like(weights_ref)
    weights_ref[0:1, 0:1 + order + count] = pen_ref[...][None, :]

    def build(h):
        table = full[0, h].reshape(LANES, LANES).T
        table = jnp.where(lax.broadcasted_iota(jnp.int32, table.shape, 1) == order, 1.0, table)
        t_hi = table.astype(jnp.bfloat16)
        both = jnp.concatenate([t_hi, (table - t_hi.astype(jnp.float32)).astype(jnp.bfloat16)], axis=1)
        rows = pl.ds(pl.multiple_of(h * LANES, LANES), LANES)

        def pick(ref, sl):
            hot = ref[:, sl]
            return dot(both, jnp.concatenate([hot, hot], axis=0), 1, 0)

        def step(at, carry):
            for u in range(CHUNK // TILE):
                sl = pl.ds(at * CHUNK + u * TILE, TILE)
                d = pick(hot_i, sl) * pick(hot_j, sl)
                d_hi = d.astype(jnp.bfloat16)
                dhi_ref[rows, sl] = d_hi
                dlo_ref[rows, sl] = (d - d_hi.astype(jnp.float32)).astype(jnp.bfloat16)
            return carry

        for at in range(padded // CHUNK):
            step(at, 0)

    collect(0)
    collect(1)
    each(spread, 0, "wait")
    relay(0).start()
    build(side)
    relay(0).wait()
    each(spread, 1, "wait")
    relay(1).start()
    build(1 - side)
    coeffs = whole(0)
    ct = coeffs.T
    inner = dot(ct, coeffs, 1, 0, highest)
    sq = coeffs * coeffs
    kernel_ref[...] = 1.0 + inner + 0.5 * (inner * inner + dot(ct * ct, sq, 1, 0, highest))
    relay(1).wait()
    rates_ref[...] = whole(1)[:order]


def fit_kernel(rates_ref, kernel_ref, dhi_ref, dlo_ref, pen_ref, out_ref, t_ref, w_ref, x_ref, pt_ref, sem):
    order, snaps = rates_ref.shape
    padded = t_ref.shape[1]
    width = x_ref.shape[1]
    g = rates_ref[...] * (1.0 / math.sqrt(snaps))
    kernel = kernel_ref[...]
    s1 = dot(g, kernel, 1, 0, highest)
    lhs = jnp.concatenate([g, s1 * (1.0 / snaps)], axis=0)
    lhs_hi = lhs.astype(jnp.bfloat16)
    lhs_lo = (lhs - lhs_hi.astype(jnp.float32)).astype(jnp.bfloat16)
    lhs_both = jnp.concatenate([lhs_hi, lhs_lo], axis=0)

    def tile(at, carry):
        tt, tw = carry
        for u in range(CHUNK // TILE):
            sl = pl.ds(at * CHUNK + u * TILE, TILE)
            both = dot(lhs_both, dhi_ref[:, sl], 1, 0)
            tv = both[:2 * order] + both[2 * order:] + dot(lhs_hi, dlo_ref[:, sl], 1, 0)
            t, v = tv[:order], tv[order:]
            pt = pen_ref[0:1, sl] * t
            w = v + pt
            t_ref[:, sl] = t
            w_ref[:, sl] = w
            pt_ref[:, sl] = pt.astype(jnp.bfloat16)
            sq, cross = t * t, t * w
            for h in range(0, TILE, LANES):
                tt = tt + sq[:, h:h + LANES]
                tw = tw + cross[:, h:h + LANES]
        return tt, tw

    zero = jnp.zeros((order, LANES), jnp.float32)
    tt, tw = zero, zero
    for at in range(padded // CHUNK):
        tt, tw = tile(at, (tt, tw))
    dpt = dot(dhi_ref[...], pt_ref[...], 1, 1)
    tt = jnp.sum(tt, axis=1, keepdims=True)
    tw = jnp.sum(tw, axis=1, keepdims=True)
    alpha = tt / tw
    ks1 = dot(s1, kernel, 1, 0, highest) * (1.0 / snaps)
    image = ks1 + jnp.pad(dpt, ((0, 0), (0, LANES - order))).T[:order]
    moved = s1 - alpha * image
    gram = jnp.sum(moved * moved, axis=1, keepdims=True) * (1.0 / snaps)
    group = 8 * max(d for d in range(1, 4) if order // 8 % d == 0)
    copies = []
    for at in range(0, order, group):
        rows = slice(at, at + group)
        a = alpha[rows]
        t, w = t_ref[rows, :], w_ref[rows, :]
        r = t - a * w
        rr = r * r
        weighted = jnp.sum(rr * pen_ref[0:1, :], axis=1, keepdims=True) + gram[rows]
        now = jnp.sum(rr, axis=1, keepdims=True)
        ratio = now / tt[rows]
        second = now / (weighted - ratio * now / a)
        x = (a + second * ratio + second) * t - (second * a) * w
        x_ref[rows, :] = x[:, :width]
        copy = pltpu.make_async_copy(x_ref.at[rows, :], out_ref.at[rows, :], sem.at[at // group])
        copy.start()
        copies.append(copy)
    for copy in copies:
        copy.wait()


def solution(mesh):
    gx, gy = mesh.shape["gx"], mesh.shape["gy"]
    pairs = gx * gy // 2

    def on_device(basis, snapshots, derivatives, quad_pairs, penalty):
        order, snaps = basis.shape[1], snapshots.shape[1]
        width = 1 + order + quad_pairs.shape[1]
        padded = -(-width // CHUNK) * CHUNK
        f32, bf16 = jnp.float32, jnp.bfloat16
        block = (pairs, LANES // pairs, LANES)
        rates, kernel, dhi, dlo, weights = pl.pallas_call(
            functools.partial(project_kernel, gx, gy),
            out_shape=[
                jax.ShapeDtypeStruct((order, snaps), f32),
                jax.ShapeDtypeStruct((snaps, snaps), f32),
                jax.ShapeDtypeStruct((snaps, padded), bf16),
                jax.ShapeDtypeStruct((snaps, padded), bf16),
                jax.ShapeDtypeStruct((1, padded), f32),
            ],
            in_specs=[HBM] * 5,
            out_specs=[VM] * 5,
            scratch_shapes=[
                pltpu.VMEM((order, basis.shape[0]), bf16),
                pltpu.VMEM(snapshots.shape, bf16),
                pltpu.VMEM(derivatives.shape, bf16),
                pltpu.VMEM(quad_pairs.shape, jnp.int32),
                pltpu.VMEM(penalty.shape, f32),
                pltpu.VMEM((2, 2) + block, f32),
                pltpu.VMEM((2,) + block, f32),
                pltpu.VMEM((2,) + block, f32),
                pltpu.VMEM((2,) + block, f32),
                pltpu.VMEM((2, 2) + block, f32),
                pltpu.VMEM((LANES, padded), bf16),
                pltpu.VMEM((LANES, padded), bf16),
                pltpu.SemaphoreType.DMA((5,)),
                pltpu.SemaphoreType.DMA((2, 4, 2, pairs)),
            ],
            compiler_params=pltpu.CompilerParams(
                collective_id=0, has_side_effects=True, vmem_limit_bytes=24 * 1024 * 1024),
            name="project",
        )(*(pltpu.with_memory_space_constraint(v, pltpu.HBM) for v in (basis.T, snapshots, derivatives, quad_pairs, penalty)))
        return pl.pallas_call(
            fit_kernel,
            out_shape=jax.ShapeDtypeStruct((order, width), f32),
            in_specs=[VM] * 5,
            out_specs=pl.BlockSpec(memory_space=pl.ANY),
            scratch_shapes=[
                pltpu.VMEM((order, padded), f32),
                pltpu.VMEM((order, padded), f32),
                pltpu.VMEM((order, width), f32),
                pltpu.VMEM((order, padded), bf16),
                pltpu.SemaphoreType.DMA((order // 8,)),
            ],
            compiler_params=pltpu.CompilerParams(vmem_limit_bytes=24 * 1024 * 1024),
            name="fit",
        )(rates, kernel, dhi, dlo, weights)

    in_specs = (P(("gx", "gy"), None), P(("gx", "gy"), None), P(("gx", "gy"), None), P(), P())
    return jax.shard_map(on_device, mesh=mesh, in_specs=in_specs, out_specs=P(), check_vma=False)
```
